256 devices in a mesh: groups: 4 (over y, x), tp: 32 (over z), sp: 2 (over core).
Axes of the slice: x: 2, y: 2, z: 32, core: 2. Of those that a mesh axis runs over, the one named last changes fastest.
The devices are a block of a 4x8x32 slice.
Arguments:
- frames: bfloat16 [1024, 1280], P(('groups', 'tp', 'sp')), parts along dimension 0, may hold values from -6 to 6
- frame_pos: int32 [1024], P(('groups', 'tp', 'sp')), parts along dimension 0, may hold values from 0 to 511, as said below
- segment_ids: int32 [2048], P(('groups', 'sp')), parts along dimension 0, may hold values from 0 to 3, as said below
- text_embed: bfloat16 [2048, 8192], P(('groups', 'sp'), 'tp'), parts along dimension 0, may hold values from -6 to 6
- pre_gain: float32 [1280], replicated, may hold values from 0.25 to 1.75
- pre_shift: float32 [1280], replicated, may hold values from -1.75 to 1.75
- expand_weight: bfloat16 [1280, 5120], P(None, 'tp'), may hold values from -0.15625 to 0.15625
- expand_bias: float32 [5120], P('tp'), may hold values from -3 to 3
- reduce_weight: bfloat16 [5120, 1280], P('tp'), may hold values from -0.078125 to 0.078125
- reduce_bias: float32 [1280], replicated, may hold values from -3 to 3
- post_gain: float32 [1280], replicated, may hold values from 0.25 to 1.75
- post_shift: float32 [1280], replicated, may hold values from -1.75 to 1.75
- projector: bfloat16 [1280, 8192], P(None, 'tp'), may hold values from -0.15625 to 0.15625
- norm_gain: float32 [8192], P('tp'), may hold values from 0.5 to 12
- query_weight: bfloat16 [8192, 8192], P(None, 'tp'), may hold values from -0.0625 to 0.0625
- key_weight: bfloat16 [8192, 1024], P('tp'), may hold values from -0.0625 to 0.0625
- value_weight: bfloat16 [8192, 1024], P('tp'), may hold values from -0.0625 to 0.0625
- output_weight: bfloat16 [8192, 8192], P('tp'), may hold values from -1 to 1
Outputs:
- hidden_states: bfloat16 [2048, 8192], P(('groups', 'sp'), 'tp'), parts along dimension 0
The draws below stay inside these ranges and needn't reach their ends.
There are 4 independent parts, one for each index of `groups`. The reference program is written for one: setup_inputs(seed, part) draws one part's arguments, and reference() takes and returns one part's arrays. A program takes and returns all parts, laid end to end along the dimension named above; an argument that names none is the same for every part. Nothing has to cross between parts.
Inputs may be any that keep to these rules, and one draw needn't show every extreme that they name: `frame_pos`: positions are distinct; each aligned run of 4 frame rows holds 4 consecutive positions starting at a multiple of 4. `segment_ids`: document numbers never fall along the prompt, and every number occurs.
All inputs are finite; a program needn't handle non-finite values.
Results may differ from the reference program's by a relative error of at most 0.034.
The reference program's roundings to bfloat16 on the way count: a program that leaves them out, or rounds other values in their place, can miss the bound.
Values may be sent and summed in bfloat16 or wider, within the bound.
No kernel may reach another device: no remote copies, remote signals or barrier semaphores. Data moves between devices by JAX's collectives and lax.ppermute only.
A program may use at most 64 MiB of HBM per device.

```python
import math
import jax
import jax.numpy as jnp
from jax import lax

D = 8192
NH = 64
KVH = 8
HD = 128
EW = 1280
EFF = 5120
CLIP = 4
SEGS = 4
LENGTH = 512
FRAMES = 256


def packing(key):
    run_count = FRAMES // CLIP
    slot_count = LENGTH // CLIP
    text_count = slot_count - run_count
    run_ids = jnp.arange(run_count, dtype=jnp.int32)
    opens = (jax.random.randint(jax.random.fold_in(key, 21), (run_count,), 0, 8) == 0) | (run_ids == 0)
    latest = lax.cummax(jnp.where(opens, run_ids, 0), axis=0)
    picks = jax.random.randint(jax.random.fold_in(key, 22), (text_count,), 0, run_count + 1)
    spread_gap = jnp.where(picks == run_count, run_count, jnp.take(latest, jnp.minimum(picks, run_count - 1)))
    side = jax.random.randint(jax.random.fold_in(key, 23), (), 0, 2)
    piled = jax.random.randint(jax.random.fold_in(key, 24), (text_count,), 0, 2) == 0
    gaps = jnp.where(piled, side * run_count, spread_gap)
    item_keys = jnp.concatenate([2 * run_ids + 1, 2 * gaps]) * slot_count + jnp.arange(slot_count, dtype=jnp.int32)
    order = jnp.argsort(item_keys).astype(jnp.int32)
    rank = jnp.argsort(order).astype(jnp.int32)
    run_slot = rank[:run_count]
    clip_score = jax.random.randint(jax.random.fold_in(key, 25), (run_count,), 0, run_count)
    row_keys = jnp.take(clip_score, latest) * run_count + run_ids
    row_runs = jnp.argsort(row_keys).astype(jnp.int32)
    row_slots = jnp.take(run_slot, row_runs)
    frame_pos = (row_slots[:, None] * CLIP + jnp.arange(CLIP, dtype=jnp.int32)[None, :]).reshape(FRAMES)
    positions = jnp.arange(LENGTH, dtype=jnp.int32)
    slot_of = positions // CLIP
    audio_slot = order < run_count
    clip_head = audio_slot & jnp.take(opens, jnp.minimum(order, run_count - 1))
    cut_ok = jnp.logical_not(jnp.take(audio_slot, slot_of)) | jnp.take(clip_head, slot_of) & (positions % CLIP == 0)
    cut_ok = cut_ok & (positions >= 1)
    raw_scores = jax.random.randint(jax.random.fold_in(key, 26), (LENGTH,), 0, LENGTH)
    scores = jnp.where(cut_ok, raw_scores * LENGTH + positions, -1)
    top_values, top_index = lax.top_k(scores, SEGS - 1)
    bounds = top_values % LENGTH
    segment_ids = jnp.sum((positions[:, None] >= bounds[None, :]).astype(jnp.int32), axis=1).astype(jnp.int32)
    return (frame_pos.astype(jnp.int32), segment_ids)


def draw_frame_pos(key, part):
    return packing(jax.random.fold_in(key, 11))[0]


def draw_segment_ids(key, part):
    return packing(jax.random.fold_in(key, 11))[1]


def draw_norm_gain(key, part):
    return jax.random.uniform(jax.random.fold_in(key, 5), (D,), jnp.float32, 0.5, 1.5)


def with_spikes(entries, own_key, source, target, blocks, factor):
    def block_of(axis_at):
        return (jnp.arange(entries.shape[axis_at]) // (entries.shape[axis_at] // blocks)).reshape((-1,) + (1,) * (entries.ndim - 1 - axis_at))

    one_side = jax.random.permutation(own_key, blocks)[block_of(target)]
    far = (block_of(target) + blocks // 2) % blocks
    return jnp.where((block_of(source) == one_side) | (block_of(source) == far), factor * entries, entries)


def block_levels(own_key, extent, shards, least, high):
    loudness = 1.0
    for position, shards_of in shards:
        heights = jax.random.uniform(jax.random.fold_in(jax.random.fold_in(own_key, 6), position), (shards_of,), jnp.float32, least / len(shards), high / len(shards))
        loudness = loudness * jnp.repeat(jnp.exp(heights), extent[position] // shards_of).reshape((-1,) + (1,) * (len(extent) - 1 - position))
    return loudness


def gaussian(own_key, extent, scale, limit, cuts=(), kind=jnp.bfloat16):
    drawn = scale * jax.random.normal(own_key, extent, jnp.float32)
    if cuts:
        drawn = drawn * block_levels(own_key, extent, cuts, -0.22, 0.18)
    return jnp.clip(drawn, -limit, limit).astype(kind)


def noise_with(stream_key, shape, scale, most, split, heavy, kind=jnp.bfloat16):
    drawn = scale * jax.random.normal(stream_key, shape, jnp.float32)
    if split:
        drawn = drawn * block_levels(stream_key, shape, split, -0.22, 0.18)
    return jnp.clip(with_spikes(drawn, jax.random.fold_in(stream_key, 3), *heavy), -most, most).astype(kind)


def setup_inputs(seed: int = 0, part: int = 0) -> dict:
    streams_of = jax.random.split(jax.random.key(seed), 19)
    own_keys = jax.random.split(jax.random.fold_in(streams_of[18], part), 19)
    return {
        "frames": gaussian(own_keys[0], (FRAMES, EW), 1.0, 6.0, ((0, 64),)),
        "frame_pos": draw_frame_pos(jax.random.fold_in(jax.random.fold_in(streams_of[18], part), 71), part),
        "segment_ids": draw_segment_ids(jax.random.fold_in(jax.random.fold_in(streams_of[18], part), 71), part),
        "text_embed": gaussian(own_keys[3], (LENGTH, D), 1.0, 6.0, ((0, 2), (1, 32))),
        "pre_gain": jnp.clip(1.0 + 0.15 * jax.random.normal(streams_of[4], (EW,), jnp.float32), 0.25, 1.75),
        "pre_shift": gaussian(streams_of[5], (EW,), 0.3, 1.75, (), jnp.float32),
        "expand_weight": gaussian(streams_of[6], (EW, EFF), EW ** -0.5, 0.15625, ((1, 32),)),
        "expand_bias": gaussian(streams_of[7], (EFF,), 0.5, 3.0, ((0, 32),), jnp.float32),
        "reduce_weight": gaussian(streams_of[8], (EFF, EW), EFF ** -0.5, 0.078125, ((0, 32),)),
        "reduce_bias": gaussian(streams_of[9], (EW,), 0.5, 3.0, (), jnp.float32),
        "post_gain": jnp.clip(1.0 + 0.15 * jax.random.normal(streams_of[10], (EW,), jnp.float32), 0.25, 1.75),
        "post_shift": gaussian(streams_of[11], (EW,), 0.3, 1.75, (), jnp.float32),
        "projector": gaussian(streams_of[12], (EW, D), EW ** -0.5, 0.15625, ((1, 32),)),
        "norm_gain": draw_norm_gain(jax.random.fold_in(streams_of[18], 71), part),
        "query_weight": gaussian(streams_of[14], (D, NH * HD), D ** -0.5, 0.0625, ((1, 32),)),
        "key_weight": gaussian(streams_of[15], (D, KVH * HD), D ** -0.5, 0.0625, ((0, 32),)),
        "value_weight": gaussian(streams_of[16], (D, KVH * HD), D ** -0.5, 0.0625, ((0, 32),)),
        "output_weight": noise_with(streams_of[17], (NH * HD, D), HD ** -0.5, 1.0, ((0, 32),), (0, 1, 32, 2.75)),
    }


rope_base = 500000.0
norm_eps = 1e-05

def layer_norm(values, gain, shift):
    widened = values.astype(jnp.float32)
    average = lax.optimization_barrier(jnp.mean(widened, axis=-1, keepdims=True))
    centred = widened - average
    spread = lax.optimization_barrier(jnp.mean(centred * centred, axis=-1, keepdims=True))
    return centred * lax.rsqrt(spread + norm_eps) * gain + shift

def rotate(values, positions):
    width = values.shape[-1]
    half_width = width // 2
    freq_index = jnp.arange(half_width).astype(jnp.float32)
    inverse = jnp.exp(freq_index * (-2.0 * math.log(rope_base) / width))
    angles = positions.astype(jnp.float32)[:, None] * inverse[None, :]
    cosine = jnp.cos(angles)[:, None, :]
    sine_part = jnp.sin(angles)[:, None, :]
    first = values[..., :half_width]
    second = values[..., half_width:]
    return jnp.concatenate([first * cosine - second * sine_part, second * cosine + first * sine_part], axis=-1)

def reference(frames, frame_pos, segment_ids, text_embed, pre_gain, pre_shift, expand_weight, expand_bias, reduce_weight, reduce_bias, post_gain, post_shift, projector, norm_gain, query_weight, key_weight, value_weight, output_weight):
    normed = layer_norm(frames, pre_gain, pre_shift).astype(jnp.bfloat16)
    inner = jnp.dot(normed, expand_weight, preferred_element_type=jnp.float32) + expand_bias
    inner = jax.nn.gelu(inner, approximate=False).astype(jnp.bfloat16)
    encoded = frames.astype(jnp.float32) + jnp.dot(inner, reduce_weight, preferred_element_type=jnp.float32) + reduce_bias
    encoded = layer_norm(encoded, post_gain, post_shift).astype(jnp.bfloat16)
    projected = jnp.dot(encoded, projector, preferred_element_type=jnp.float32).astype(jnp.bfloat16)
    stream = text_embed.at[frame_pos].set(projected)
    widened = stream.astype(jnp.float32)
    sum_squares = lax.optimization_barrier(jnp.sum(widened * widened, axis=1, keepdims=True))
    normed_stream = (widened * lax.rsqrt(sum_squares / D + norm_eps) * norm_gain).astype(jnp.bfloat16)
    positions = jnp.arange(LENGTH)
    query_raw = jnp.dot(normed_stream, query_weight, preferred_element_type=jnp.float32).astype(jnp.bfloat16)
    key_raw = jnp.dot(normed_stream, key_weight, preferred_element_type=jnp.float32).astype(jnp.bfloat16)
    value_rows = jnp.dot(normed_stream, value_weight, preferred_element_type=jnp.float32).astype(jnp.bfloat16)
    queries = rotate(lax.optimization_barrier(query_raw).astype(jnp.float32).reshape(LENGTH, NH, HD), positions).astype(jnp.bfloat16)
    key_rows = rotate(lax.optimization_barrier(key_raw).astype(jnp.float32).reshape(LENGTH, KVH, HD), positions).astype(jnp.bfloat16)
    value_rows = value_rows.reshape(LENGTH, KVH, HD)
    allowed = (positions[None, :] <= positions[:, None]) & (segment_ids[None, :] == segment_ids[:, None])
    group_size = NH // KVH
    inv_scale = 1.0 / math.sqrt(HD)

    def one_head(head_index):
        head_queries = queries[:, head_index, :]
        head_keys = key_rows[:, head_index // group_size, :]
        head_values = value_rows[:, head_index // group_size, :]
        scores = jnp.dot(head_queries, head_keys.T, preferred_element_type=jnp.float32) * inv_scale
        scores = jnp.where(allowed, scores, -1e+30)
        row_max = lax.optimization_barrier(jnp.max(scores, axis=1, keepdims=True))
        expo = jnp.where(allowed, jnp.exp(scores - row_max), 0.0)
        denom = lax.optimization_barrier(jnp.sum(expo, axis=1, keepdims=True))
        mixed = jnp.dot(expo.astype(jnp.bfloat16), head_values, preferred_element_type=jnp.float32) / denom
        return mixed.astype(jnp.bfloat16)
    per_head = lax.map(one_head, jnp.arange(NH))
    attended = jnp.transpose(per_head, (1, 0, 2)).reshape(LENGTH, NH * HD)
    mixed = jnp.dot(attended, output_weight, preferred_element_type=jnp.float32)
    return (widened + mixed).astype(jnp.bfloat16)
```

```python
import math

import jax
import jax.numpy as jnp
from jax import lax
from jax.experimental import pallas as pl
from jax.experimental.pallas import tpu as pltpu
from jax.sharding import PartitionSpec as P

D = 8192
NH = 64
KVH = 8
HD = 128


rope_base = 500000.0
norm_eps = 1e-05


def swapped(value):
    return lax.ppermute(value, "sp", [(0, 1), (1, 0)])


def in_three(values):
    high = lax.reduce_precision(values, 8, 7)
    middle = lax.reduce_precision(values - high, 8, 7)
    low = values - high - middle
    return jnp.stack([high, middle, low]).astype(jnp.bfloat16)


def query_kernel(width, rows, shard_ref, gathered, encoded, placing, is_audio, weight, query, squares):
    @pl.when(pl.program_id(0) == 0)
    def _():
        query[...] = jnp.zeros_like(query)
        squares[...] = jnp.zeros_like(squares)

    def both(first, last):
        return jnp.concatenate([gathered[0, first:last, :], gathered[1, first:last, :]], axis=1)

    projected = jnp.dot(
        encoded[...], both(0, width), preferred_element_type=jnp.float32
    ).astype(jnp.bfloat16)
    placed = jnp.dot(placing[...], projected, preferred_element_type=jnp.float32)
    text = both(width, width + rows).astype(jnp.float32)
    stream = jnp.where(is_audio[...] > 0.0, placed, text)
    half = squares.shape[1]
    squared = stream * stream
    squares[...] += squared[:, :half] + squared[:, half:]
    parts = both(width + rows, width + rows + 16).astype(jnp.float32)
    gain = parts[0:1] + parts[1:2] + parts[2:3]
    scaled = (stream * gain).astype(jnp.bfloat16)
    query[...] += jnp.dot(
        scaled, weight[...].reshape(scaled.shape[1], query.shape[1]), preferred_element_type=jnp.float32
    )


def query_partial(shard, gathered, encoded, placing, is_audio, weight):
    chips, height, half = gathered.shape
    frames, width = encoded.shape
    rows = placing.shape[0]
    columns = weight.shape[-1]
    grid_spec = pltpu.PrefetchScalarGridSpec(
        num_scalar_prefetch=1,
        grid=(chips // 2,),
        in_specs=[
            pl.BlockSpec((2, height, half), lambda g, s: (g, 0, 0)),
            pl.BlockSpec((frames, width), lambda g, s: (0, 0)),
            pl.BlockSpec((rows, frames), lambda g, s: (0, 0)),
            pl.BlockSpec((rows, 1), lambda g, s: (0, 0)),
            pl.BlockSpec((2, 1, half, columns), lambda g, s: (g, s[0], 0, 0)),
        ],
        out_specs=[
            pl.BlockSpec((rows, columns), lambda g, s: (0, 0)),
            pl.BlockSpec((rows, half), lambda g, s: (0, 0)),
        ],
    )
    features = chips * half
    return pl.pallas_call(
        lambda *refs: query_kernel(width, rows, *refs),
        grid_spec=grid_spec,
        out_shape=[
            jax.ShapeDtypeStruct((rows, columns), jnp.float32),
            jax.ShapeDtypeStruct((rows, half), jnp.float32),
        ],
        compiler_params=pltpu.CompilerParams(dimension_semantics=("arbitrary",)),
        cost_estimate=pl.CostEstimate(
            flops=2 * features * (frames * width + rows * frames + rows * columns),
            bytes_accessed=2 * gathered.size,
            transcendentals=0,
        ),
        name="query_partial",
    )(shard.reshape(1), gathered, encoded, placing, is_audio, weight)


def layer_norm(values, gain, shift):
    widened = values.astype(jnp.float32)
    average = jnp.mean(widened, axis=-1, keepdims=True)
    centred = widened - average
    spread = jnp.mean(centred * centred, axis=-1, keepdims=True)
    return centred * lax.rsqrt(spread + norm_eps) * gain + shift


def rotate(values, positions):
    width = values.shape[-1]
    half_width = width // 2
    freq_index = jnp.arange(half_width).astype(jnp.float32)
    inverse = jnp.exp(freq_index * (-2.0 * math.log(rope_base) / width))
    angles = positions.astype(jnp.float32)[:, None] * inverse[None, :]
    cosine = jnp.cos(angles)[:, None, :]
    sine_part = jnp.sin(angles)[:, None, :]
    first = values[..., :half_width]
    second = values[..., half_width:]
    return jnp.concatenate(
        [first * cosine - second * sine_part, second * cosine + first * sine_part], axis=-1
    )


def per_device(
    frames,
    frame_pos,
    segment_ids,
    text_embed,
    pre_gain,
    pre_shift,
    expand_weight,
    expand_bias,
    reduce_weight,
    reduce_bias,
    post_gain,
    post_shift,
    projector,
    norm_gain,
    query_weight,
    key_weight,
    value_weight,
    output_weight,
):
    seq_rows, width = text_embed.shape
    half = width // 2
    shard = lax.axis_index("sp").astype(jnp.int32)
    chips = lax.axis_size("tp")
    mine = lax.dynamic_slice_in_dim(text_embed, shard * half, half, 1)
    theirs = swapped(lax.dynamic_slice_in_dim(text_embed, (1 - shard) * half, half, 1))
    other_segs = swapped(segment_ids)
    low = shard == 0
    text_half = jnp.concatenate([jnp.where(low, mine, theirs), jnp.where(low, theirs, mine)])
    key_segs = jnp.concatenate(
        [jnp.where(low, segment_ids, other_segs), jnp.where(low, other_segs, segment_ids)]
    )
    gains = in_three(lax.dynamic_slice_in_dim(norm_gain, shard * half, half, 0))
    gathered = lax.all_gather(
        jnp.concatenate(
            [
                lax.dynamic_slice_in_dim(projector, shard * half, half, 1),
                text_half,
                jnp.pad(gains, ((0, 13), (0, 0))),
            ]
        ),
        "tp",
        axis=0,
    )
    normed = layer_norm(frames, pre_gain, pre_shift).astype(jnp.bfloat16)
    inner = (
        jnp.dot(
            lax.all_gather(normed, "tp", axis=0, tiled=True),
            expand_weight,
            preferred_element_type=jnp.float32,
        )
        + expand_bias
    )
    inner_all = jax.nn.gelu(inner, approximate=False).astype(jnp.bfloat16)
    parts = jnp.dot(inner_all, reduce_weight, preferred_element_type=jnp.float32).astype(
        jnp.bfloat16
    )
    arrived = lax.all_to_all(parts.reshape(chips, -1, parts.shape[1]), "tp", 0, 0, tiled=True)
    summed = arrived.astype(jnp.float32).sum(axis=0)
    encoded = frames.astype(jnp.float32) + summed + reduce_bias
    encoded = layer_norm(encoded, post_gain, post_shift).astype(jnp.bfloat16)
    enc_width = encoded.shape[1]
    where_to = jnp.stack([frame_pos // 256, frame_pos % 256], axis=1).astype(jnp.bfloat16)
    labelled = jnp.concatenate([encoded, jnp.pad(where_to, ((0, 0), (0, 126)))], axis=1)
    labelled = lax.all_gather(labelled, "tp", axis=0, tiled=True)
    labelled = lax.all_gather(labelled, "sp", axis=0, tiled=True)
    audio = labelled[:, :enc_width]
    pos_parts = labelled[:, enc_width : enc_width + 2].astype(jnp.float32)
    audio_pos = (pos_parts[:, 0] * 256.0 + pos_parts[:, 1]).astype(jnp.int32)
    projected = jnp.dot(audio, projector, preferred_element_type=jnp.float32).astype(jnp.bfloat16)
    positions = shard * seq_rows + jnp.arange(seq_rows, dtype=jnp.int32)
    placing = positions[:, None] == audio_pos[None, :]
    placed = jnp.dot(
        placing.astype(jnp.bfloat16), projected, preferred_element_type=jnp.float32
    ).astype(jnp.bfloat16)
    stream = jnp.where(jnp.any(placing, axis=1)[:, None], placed, text_embed)
    widened = stream.astype(jnp.float32)
    scaled = (widened * norm_gain).astype(jnp.bfloat16)
    key_part = jnp.dot(scaled, key_weight, preferred_element_type=jnp.float32)
    value_part = jnp.dot(scaled, value_weight, preferred_element_type=jnp.float32)
    key_total, value_total = lax.psum((key_part, value_part), "tp")
    shared_head = lax.axis_index("tp") * (query_weight.shape[1] // HD) // (NH // KVH)
    key_mine = lax.dynamic_slice_in_dim(key_total, shared_head * HD, HD, 1).astype(jnp.bfloat16)
    value_mine = lax.dynamic_slice_in_dim(value_total, shared_head * HD, HD, 1).astype(jnp.bfloat16)
    key_mine, value_mine, audio_pos, audio = lax.optimization_barrier(
        (key_mine, value_mine, audio_pos, audio)
    )
    all_rows = jnp.arange(key_segs.shape[0], dtype=jnp.int32)
    placing_all = all_rows[:, None] == audio_pos[None, :]
    is_audio = jnp.any(placing_all, axis=1)[:, None].astype(jnp.float32)
    heads_here = query_weight.shape[1] // HD
    query_sums, square_sums = query_partial(
        shard,
        gathered,
        audio,
        placing_all.astype(jnp.bfloat16),
        is_audio,
        query_weight.reshape(chips, 2, half, query_weight.shape[1]),
    )
    both_sums = jnp.concatenate([query_sums, square_sums], axis=1)
    own = lax.dynamic_slice_in_dim(both_sums, shard * seq_rows, seq_rows, 0)
    sent = lax.dynamic_slice_in_dim(both_sums, (1 - shard) * seq_rows, seq_rows, 0)
    own = own + swapped(sent)
    columns = query_weight.shape[1]
    inverse_rms = lax.rsqrt(jnp.sum(own[:, columns:], axis=1, keepdims=True) / D + norm_eps)
    query_raw = own[:, :columns] * inverse_rms
    queries = rotate(
        lax.optimization_barrier(query_raw.astype(jnp.bfloat16))
        .astype(jnp.float32)
        .reshape(seq_rows, heads_here, HD),
        positions,
    ).astype(jnp.bfloat16)
    key_mine = (key_mine.astype(jnp.float32) * inverse_rms).astype(jnp.bfloat16)
    value_mine = (value_mine.astype(jnp.float32) * inverse_rms).astype(jnp.bfloat16)
    key_rows = rotate(
        lax.optimization_barrier(key_mine).astype(jnp.float32)[:, None, :], positions
    )[:, 0, :].astype(jnp.bfloat16)
    both_rows = lax.all_gather(
        jnp.concatenate([key_rows, value_mine], axis=1), "sp", axis=0, tiled=True
    )
    key_block = both_rows[:, :HD]
    value_block = both_rows[:, HD:]
    inv_scale = 1.0 / math.sqrt(HD)
    running_max = jnp.full((heads_here, seq_rows), -1e30, jnp.float32)
    key_pos = jnp.arange(key_block.shape[0], dtype=jnp.int32)
    allowed = (key_pos[None, :] <= positions[:, None]) & (key_segs[None, :] == segment_ids[:, None])
    scores = (
        jnp.einsum("qhd,kd->hqk", queries, key_block, preferred_element_type=jnp.float32)
        * inv_scale
    )
    scores = jnp.where(allowed[None], scores, -1e30)
    new_max = jnp.maximum(running_max, jnp.max(scores, axis=2))
    expo = jnp.where(allowed[None], jnp.exp(scores - new_max[:, :, None]), 0.0)
    weight_sum = jnp.sum(expo, axis=2)
    accum = jnp.einsum(
        "hqk,kd->qhd", expo.astype(jnp.bfloat16), value_block, preferred_element_type=jnp.float32
    )
    running_max, weight_sum, accum = (new_max, weight_sum, accum)
    attended = (
        (accum / jnp.transpose(weight_sum)[:, :, None])
        .astype(jnp.bfloat16)
        .reshape(seq_rows, heads_here * HD)
    )
    block = output_weight
    mixed = jnp.transpose(
        lax.psum_scatter(
            jnp.einsum("hd,qh->dq", block, attended, preferred_element_type=jnp.float32).astype(
                jnp.bfloat16
            ),
            "tp",
            scatter_dimension=0,
            tiled=True,
        ).astype(jnp.float32)
    )
    return (widened + mixed).astype(jnp.bfloat16)


def solution(mesh):
    return jax.shard_map(
        per_device,
        mesh=mesh,
        in_specs=(
            P(("groups", "tp", "sp"), None),
            P(("groups", "tp", "sp")),
            P(("groups", "sp")),
            P(("groups", "sp"), "tp"),
            P(),
            P(),
            P(None, "tp"),
            P("tp"),
            P("tp", None),
            P(),
            P(),
            P(),
            P(None, "tp"),
            P("tp"),
            P(None, "tp"),
            P("tp", None),
            P("tp", None),
            P("tp", None),
        ),
        out_specs=P(("groups", "sp"), "tp"),
        check_vma=False,
    )
```

```python
import math

import jax
import jax.numpy as jnp
from jax import lax
from jax.experimental import pallas as pl
from jax.experimental.pallas import tpu as pltpu
from jax.sharding import PartitionSpec as P

D = 8192
NH = 64
KVH = 8
HD = 128


rope_base = 500000.0
norm_eps = 1e-05


def swapped(value):
    return lax.ppermute(value, "sp", [(0, 1), (1, 0)])


def in_three(values):
    high = lax.reduce_precision(values, 8, 7)
    middle = lax.reduce_precision(values - high, 8, 7)
    low = values - high - middle
    return jnp.stack([high, middle, low]).astype(jnp.bfloat16)


TOGETHER = 4


def query_kernel(rows, text_ref, late, placing, is_audio, weight, query, squares):
    @pl.when(pl.program_id(0) == 0)
    def _():
        query[...] = jnp.zeros_like(query)
        squares[...] = jnp.zeros_like(squares)

    def side_by_side(ref, first, last):
        return jnp.concatenate([ref[k, first:last, :] for k in range(TOGETHER)], axis=1)

    projected = side_by_side(late, 0, late.shape[1])
    placed = jnp.dot(placing[...], projected, preferred_element_type=jnp.float32)
    text = side_by_side(text_ref, 0, rows).astype(jnp.float32)
    stream = jnp.where(is_audio[...] > 0.0, placed, text)
    half = squares.shape[1]
    squared = stream * stream
    squares[...] += sum(squared[:, k * half : (k + 1) * half] for k in range(TOGETHER))
    parts = side_by_side(text_ref, rows, rows + 16).astype(jnp.float32)
    gain = parts[0:1] + parts[1:2] + parts[2:3]
    scaled = (stream * gain).astype(jnp.bfloat16)
    query[...] += jnp.dot(
        scaled,
        weight[...].reshape(scaled.shape[1], query.shape[1]),
        preferred_element_type=jnp.float32,
    )


def query_partial(shard, early, late, placing, is_audio, weight):
    chips, height, half = early.shape
    frames = late.shape[1]
    rows = placing.shape[0]
    columns = weight.shape[-1]
    grid_spec = pltpu.PrefetchScalarGridSpec(
        num_scalar_prefetch=1,
        grid=(chips // TOGETHER,),
        in_specs=[
            pl.BlockSpec((TOGETHER, height, half), lambda g, s: (g, 0, 0)),
            pl.BlockSpec((TOGETHER, frames, half), lambda g, s: (g, 0, 0)),
            pl.BlockSpec((rows, frames), lambda g, s: (0, 0)),
            pl.BlockSpec((rows, 1), lambda g, s: (0, 0)),
            pl.BlockSpec((TOGETHER, 1, half, columns), lambda g, s: (g, s[0], 0, 0)),
        ],
        out_specs=[
            pl.BlockSpec((rows, columns), lambda g, s: (0, 0)),
            pl.BlockSpec((rows, half), lambda g, s: (0, 0)),
        ],
    )

    def kernel(shard_ref, *refs):
        query_kernel(rows, *refs)

    return pl.pallas_call(
        kernel,
        grid_spec=grid_spec,
        out_shape=[
            jax.ShapeDtypeStruct((rows, columns), jnp.float32),
            jax.ShapeDtypeStruct((rows, half), jnp.float32),
        ],
        compiler_params=pltpu.CompilerParams(dimension_semantics=("arbitrary",)),
        cost_estimate=pl.CostEstimate(
            flops=2 * chips * half * rows * (frames + columns),
            bytes_accessed=2 * (early.size + late.size),
            transcendentals=0,
        ),
        name="query_partial",
    )(shard.reshape(1), early, late, placing, is_audio, weight)


def layer_norm(values, gain, shift):
    widened = values.astype(jnp.float32)
    average = jnp.mean(widened, axis=-1, keepdims=True)
    centred = widened - average
    spread = jnp.mean(centred * centred, axis=-1, keepdims=True)
    return centred * lax.rsqrt(spread + norm_eps) * gain + shift


def rotate(values, positions):
    width = values.shape[-1]
    half_width = width // 2
    freq_index = jnp.arange(half_width).astype(jnp.float32)
    inverse = jnp.exp(freq_index * (-2.0 * math.log(rope_base) / width))
    angles = positions.astype(jnp.float32)[:, None] * inverse[None, :]
    cosine = jnp.cos(angles)[:, None, :]
    sine_part = jnp.sin(angles)[:, None, :]
    first = values[..., :half_width]
    second = values[..., half_width:]
    return jnp.concatenate(
        [first * cosine - second * sine_part, second * cosine + first * sine_part], axis=-1
    )


def per_device(
    frames,
    frame_pos,
    segment_ids,
    text_embed,
    pre_gain,
    pre_shift,
    expand_weight,
    expand_bias,
    reduce_weight,
    reduce_bias,
    post_gain,
    post_shift,
    projector,
    norm_gain,
    query_weight,
    key_weight,
    value_weight,
    output_weight,
):
    seq_rows, width = text_embed.shape
    half = width // 2
    shard = lax.axis_index("sp").astype(jnp.int32)
    chips = lax.axis_size("tp")
    mine = lax.dynamic_slice_in_dim(text_embed, shard * half, half, 1)
    theirs = swapped(lax.dynamic_slice_in_dim(text_embed, (1 - shard) * half, half, 1))
    other_segs = swapped(segment_ids)
    low = shard == 0
    text_half = jnp.concatenate([jnp.where(low, mine, theirs), jnp.where(low, theirs, mine)])
    key_segs = jnp.concatenate(
        [jnp.where(low, segment_ids, other_segs), jnp.where(low, other_segs, segment_ids)]
    )
    gains = in_three(lax.dynamic_slice_in_dim(norm_gain, shard * half, half, 0))
    normed = layer_norm(frames, pre_gain, pre_shift).astype(jnp.bfloat16)
    early, normed = lax.optimization_barrier(
        (jnp.concatenate([text_half, jnp.pad(gains, ((0, 13), (0, 0)))]), normed)
    )
    early = lax.all_gather(early, "tp", axis=0)
    inner = (
        jnp.dot(
            lax.all_gather(normed, "tp", axis=0, tiled=True),
            expand_weight,
            preferred_element_type=jnp.float32,
        )
        + expand_bias
    )
    inner_all = jax.nn.gelu(inner, approximate=False).astype(jnp.bfloat16)
    parts = jnp.dot(inner_all, reduce_weight, preferred_element_type=jnp.float32).astype(
        jnp.bfloat16
    )
    arrived = lax.all_to_all(parts.reshape(chips, -1, parts.shape[1]), "tp", 0, 0, tiled=True)
    summed = arrived.astype(jnp.float32).sum(axis=0)
    encoded = frames.astype(jnp.float32) + summed + reduce_bias
    encoded = layer_norm(encoded, post_gain, post_shift).astype(jnp.bfloat16)
    enc_width = encoded.shape[1]
    where_to = jnp.stack([frame_pos // 256, frame_pos % 256], axis=1).astype(jnp.bfloat16)
    labelled = jnp.concatenate([encoded, jnp.pad(where_to, ((0, 0), (0, 126)))], axis=1)
    by_head = jnp.concatenate(
        [
            weight[:, k * HD : (k + 1) * HD]
            for k in range(KVH)
            for weight in (key_weight, value_weight)
        ],
        axis=1,
    )
    labelled, by_head = lax.optimization_barrier((labelled, by_head))
    labelled = lax.all_gather(labelled, "tp", axis=0, tiled=True)
    labelled = lax.all_gather(labelled, "sp", axis=0, tiled=True)
    audio = labelled[:, :enc_width]
    pos_parts = labelled[:, enc_width : enc_width + 2].astype(jnp.float32)
    audio_pos = (pos_parts[:, 0] * 256.0 + pos_parts[:, 1]).astype(jnp.int32)
    projected = jnp.dot(audio, projector, preferred_element_type=jnp.float32).astype(jnp.bfloat16)
    late = lax.dynamic_slice_in_dim(projected, shard * half, half, 1)
    early, late = lax.optimization_barrier((early, late))
    late = lax.all_gather(late, "tp", axis=0)
    positions = shard * seq_rows + jnp.arange(seq_rows, dtype=jnp.int32)
    placing = positions[:, None] == audio_pos[None, :]
    placed = jnp.dot(
        placing.astype(jnp.bfloat16), projected, preferred_element_type=jnp.float32
    ).astype(jnp.bfloat16)
    stream = jnp.where(jnp.any(placing, axis=1)[:, None], placed, text_embed)
    widened = stream.astype(jnp.float32)
    scaled = (widened * norm_gain).astype(jnp.bfloat16)
    sharers = chips // KVH
    quads = [[sharers * k + m for m in range(sharers)] for k in range(KVH)]
    strides = [[sharers * k + m for k in range(KVH)] for m in range(sharers)]
    shared = jnp.dot(scaled, by_head, preferred_element_type=jnp.float32).astype(jnp.bfloat16)
    shared = lax.all_to_all(
        shared.reshape(sharers, seq_rows // sharers, -1), "tp", 0, 0, axis_index_groups=quads, tiled=True
    )
    shared = shared.astype(jnp.float32).sum(axis=0).astype(jnp.bfloat16)
    shared = jnp.stack([shared[:, 2 * HD * k : 2 * HD * (k + 1)] for k in range(KVH)])
    shared = lax.all_to_all(shared, "tp", 0, 0, axis_index_groups=strides, tiled=True)
    shared = shared.astype(jnp.float32).sum(axis=0).astype(jnp.bfloat16)
    shared = lax.all_gather(shared, "tp", axis=0, tiled=True, axis_index_groups=quads)
    key_mine = shared[:, :HD]
    value_mine = shared[:, HD:]
    key_mine, value_mine, audio_pos = lax.optimization_barrier((key_mine, value_mine, audio_pos))
    all_rows = jnp.arange(key_segs.shape[0], dtype=jnp.int32)
    placing_all = all_rows[:, None] == audio_pos[None, :]
    is_audio = jnp.any(placing_all, axis=1)[:, None].astype(jnp.float32)
    heads_here = query_weight.shape[1] // HD
    query_sums, square_sums = query_partial(
        shard,
        early,
        late,
        placing_all.astype(jnp.bfloat16),
        is_audio,
        query_weight.reshape(chips, 2, half, query_weight.shape[1]),
    )
    both_sums = jnp.concatenate([query_sums, square_sums], axis=1)
    own = lax.dynamic_slice_in_dim(both_sums, shard * seq_rows, seq_rows, 0)
    sent = lax.dynamic_slice_in_dim(both_sums, (1 - shard) * seq_rows, seq_rows, 0)
    own = own + swapped(sent)
    columns = query_weight.shape[1]
    inverse_rms = lax.rsqrt(jnp.sum(own[:, columns:], axis=1, keepdims=True) / D + norm_eps)
    query_raw = own[:, :columns] * inverse_rms
    queries = rotate(
        lax.optimization_barrier(query_raw.astype(jnp.bfloat16))
        .astype(jnp.float32)
        .reshape(seq_rows, heads_here, HD),
        positions,
    ).astype(jnp.bfloat16)
    key_mine = (key_mine.astype(jnp.float32) * inverse_rms).astype(jnp.bfloat16)
    value_mine = (value_mine.astype(jnp.float32) * inverse_rms).astype(jnp.bfloat16)
    key_rows = rotate(
        lax.optimization_barrier(key_mine).astype(jnp.float32)[:, None, :], positions
    )[:, 0, :].astype(jnp.bfloat16)
    both_rows = lax.all_gather(
        jnp.concatenate([key_rows, value_mine], axis=1), "sp", axis=0, tiled=True
    )
    key_block = both_rows[:, :HD]
    value_block = both_rows[:, HD:]
    inv_scale = 1.0 / math.sqrt(HD)
    running_max = jnp.full((heads_here, seq_rows), -1e30, jnp.float32)
    key_pos = jnp.arange(key_block.shape[0], dtype=jnp.int32)
    allowed = (key_pos[None, :] <= positions[:, None]) & (key_segs[None, :] == segment_ids[:, None])
    scores = (
        jnp.einsum("qhd,kd->hqk", queries, key_block, preferred_element_type=jnp.float32)
        * inv_scale
    )
    scores = jnp.where(allowed[None], scores, -1e30)
    new_max = jnp.maximum(running_max, jnp.max(scores, axis=2))
    expo = jnp.where(allowed[None], jnp.exp(scores - new_max[:, :, None]), 0.0)
    weight_sum = jnp.sum(expo, axis=2)
    accum = jnp.einsum(
        "hqk,kd->qhd", expo.astype(jnp.bfloat16), value_block, preferred_element_type=jnp.float32
    )
    running_max, weight_sum, accum = (new_max, weight_sum, accum)
    attended = (
        (accum / jnp.transpose(weight_sum)[:, :, None])
        .astype(jnp.bfloat16)
        .reshape(seq_rows, heads_here * HD)
    )
    block = output_weight
    mixed = jnp.transpose(
        lax.psum_scatter(
            jnp.einsum("hd,qh->dq", block, attended, preferred_element_type=jnp.float32).astype(
                jnp.bfloat16
            ),
            "tp",
            scatter_dimension=0,
            tiled=True,
        ).astype(jnp.float32)
    )
    return (widened + mixed).astype(jnp.bfloat16)


def solution(mesh):
    return jax.shard_map(
        per_device,
        mesh=mesh,
        in_specs=(
            P(("groups", "tp", "sp"), None),
            P(("groups", "tp", "sp")),
            P(("groups", "sp")),
            P(("groups", "sp"), "tp"),
            P(),
            P(),
            P(None, "tp"),
            P("tp"),
            P("tp", None),
            P(),
            P(),
            P(),
            P(None, "tp"),
            P("tp"),
            P(None, "tp"),
            P("tp", None),
            P("tp", None),
            P("tp", None),
        ),
        out_specs=P(("groups", "sp"), "tp"),
        check_vma=False,
    )
```

```python
import math

import jax
import jax.numpy as jnp
from jax import lax
from jax.experimental import pallas as pl
from jax.experimental.pallas import tpu as pltpu
from jax.sharding import PartitionSpec as P

D = 8192
NH = 64
KVH = 8
HD = 128


rope_base = 500000.0
norm_eps = 1e-05


def swapped(value):
    return lax.ppermute(value, "sp", [(0, 1), (1, 0)])


def in_three(values):
    high = lax.reduce_precision(values, 8, 7)
    middle = lax.reduce_precision(values - high, 8, 7)
    low = values - high - middle
    return jnp.stack([high, middle, low]).astype(jnp.bfloat16)


def query_kernel(width, rows, shard_ref, gathered, encoded, placing, is_audio, weight, query, squares):
    @pl.when(pl.program_id(0) == 0)
    def _():
        query[...] = jnp.zeros_like(query)
        squares[...] = jnp.zeros_like(squares)

    def both(first, last):
        return jnp.concatenate([gathered[0, first:last, :], gathered[1, first:last, :]], axis=1)

    projected = jnp.dot(
        encoded[...], both(0, width), preferred_element_type=jnp.float32
    ).astype(jnp.bfloat16)
    placed = jnp.dot(placing[...], projected, preferred_element_type=jnp.float32)
    text = both(width, width + rows).astype(jnp.float32)
    stream = jnp.where(is_audio[...] > 0.0, placed, text)
    half = squares.shape[1]
    squared = stream * stream
    squares[...] += squared[:, :half] + squared[:, half:]
    parts = both(width + rows, width + rows + 16).astype(jnp.float32)
    gain = parts[0:1] + parts[1:2] + parts[2:3]
    scaled = (stream * gain).astype(jnp.bfloat16)
    query[...] += jnp.dot(
        scaled, weight[...].reshape(scaled.shape[1], query.shape[1]), preferred_element_type=jnp.float32
    )


def query_partial(shard, gathered, encoded, placing, is_audio, weight):
    chips, height, half = gathered.shape
    frames, width = encoded.shape
    rows = placing.shape[0]
    columns = weight.shape[-1]
    grid_spec = pltpu.PrefetchScalarGridSpec(
        num_scalar_prefetch=1,
        grid=(chips // 2,),
        in_specs=[
            pl.BlockSpec((2, height, half), lambda g, s: (g, 0, 0)),
            pl.BlockSpec((frames, width), lambda g, s: (0, 0)),
            pl.BlockSpec((rows, frames), lambda g, s: (0, 0)),
            pl.BlockSpec((rows, 1), lambda g, s: (0, 0)),
            pl.BlockSpec((2, 1, half, columns), lambda g, s: (g, s[0], 0, 0)),
        ],
        out_specs=[
            pl.BlockSpec((rows, columns), lambda g, s: (0, 0)),
            pl.BlockSpec((rows, half), lambda g, s: (0, 0)),
        ],
    )
    features = chips * half
    return pl.pallas_call(
        lambda *refs: query_kernel(width, rows, *refs),
        grid_spec=grid_spec,
        out_shape=[
            jax.ShapeDtypeStruct((rows, columns), jnp.float32),
            jax.ShapeDtypeStruct((rows, half), jnp.float32),
        ],
        compiler_params=pltpu.CompilerParams(dimension_semantics=("arbitrary",)),
        cost_estimate=pl.CostEstimate(
            flops=2 * features * (frames * width + rows * frames + rows * columns),
            bytes_accessed=2 * gathered.size,
            transcendentals=0,
        ),
        name="query_partial",
    )(shard.reshape(1), gathered, encoded, placing, is_audio, weight)


def layer_norm(values, gain, shift):
    widened = values.astype(jnp.float32)
    average = jnp.mean(widened, axis=-1, keepdims=True)
    centred = widened - average
    spread = jnp.mean(centred * centred, axis=-1, keepdims=True)
    return centred * lax.rsqrt(spread + norm_eps) * gain + shift


def rotate(values, positions):
    width = values.shape[-1]
    half_width = width // 2
    freq_index = jnp.arange(half_width).astype(jnp.float32)
    inverse = jnp.exp(freq_index * (-2.0 * math.log(rope_base) / width))
    angles = positions.astype(jnp.float32)[:, None] * inverse[None, :]
    cosine = jnp.cos(angles)[:, None, :]
    sine_part = jnp.sin(angles)[:, None, :]
    first = values[..., :half_width]
    second = values[..., half_width:]
    return jnp.concatenate(
        [first * cosine - second * sine_part, second * cosine + first * sine_part], axis=-1
    )


def per_device(
    frames,
    frame_pos,
    segment_ids,
    text_embed,
    pre_gain,
    pre_shift,
    expand_weight,
    expand_bias,
    reduce_weight,
    reduce_bias,
    post_gain,
    post_shift,
    projector,
    norm_gain,
    query_weight,
    key_weight,
    value_weight,
    output_weight,
):
    seq_rows, width = text_embed.shape
    half = width // 2
    shard = lax.axis_index("sp").astype(jnp.int32)
    chips = lax.axis_size("tp")
    mine = lax.dynamic_slice_in_dim(text_embed, shard * half, half, 1)
    theirs = swapped(lax.dynamic_slice_in_dim(text_embed, (1 - shard) * half, half, 1))
    other_segs = swapped(segment_ids)
    low = shard == 0
    text_half = jnp.concatenate([jnp.where(low, mine, theirs), jnp.where(low, theirs, mine)])
    key_segs = jnp.concatenate(
        [jnp.where(low, segment_ids, other_segs), jnp.where(low, other_segs, segment_ids)]
    )
    gains = in_three(lax.dynamic_slice_in_dim(norm_gain, shard * half, half, 0))
    gathered = lax.all_gather(
        jnp.concatenate(
            [
                lax.dynamic_slice_in_dim(projector, shard * half, half, 1),
                text_half,
                jnp.pad(gains, ((0, 13), (0, 0))),
            ]
        ),
        "tp",
        axis=0,
    )
    normed = layer_norm(frames, pre_gain, pre_shift).astype(jnp.bfloat16)
    inner = (
        jnp.dot(
            lax.all_gather(normed, "tp", axis=0, tiled=True),
            expand_weight,
            preferred_element_type=jnp.float32,
        )
        + expand_bias
    )
    inner_all = jax.nn.gelu(inner, approximate=False).astype(jnp.bfloat16)
    parts = jnp.dot(inner_all, reduce_weight, preferred_element_type=jnp.float32).astype(
        jnp.bfloat16
    )
    parts, key_weight, value_weight = lax.optimization_barrier((parts, key_weight, value_weight))
    by_head = jnp.concatenate(
        [
            weight[:, k * HD : (k + 1) * HD]
            for k in range(KVH)
            for weight in (key_weight, value_weight)
        ],
        axis=1,
    )
    arrived = lax.all_to_all(parts.reshape(chips, -1, parts.shape[1]), "tp", 0, 0, tiled=True)
    summed = arrived.astype(jnp.float32).sum(axis=0)
    encoded = frames.astype(jnp.float32) + summed + reduce_bias
    encoded = layer_norm(encoded, post_gain, post_shift).astype(jnp.bfloat16)
    enc_width = encoded.shape[1]
    where_to = jnp.stack([frame_pos // 256, frame_pos % 256], axis=1).astype(jnp.bfloat16)
    labelled = jnp.concatenate([encoded, jnp.pad(where_to, ((0, 0), (0, 126)))], axis=1)
    labelled, by_head = lax.optimization_barrier((labelled, by_head))
    labelled = lax.all_gather(labelled, "tp", axis=0, tiled=True)
    labelled = lax.all_gather(labelled, "sp", axis=0, tiled=True)
    audio = labelled[:, :enc_width]
    pos_parts = labelled[:, enc_width : enc_width + 2].astype(jnp.float32)
    audio_pos = (pos_parts[:, 0] * 256.0 + pos_parts[:, 1]).astype(jnp.int32)
    projected = jnp.dot(audio, projector, preferred_element_type=jnp.float32).astype(jnp.bfloat16)
    positions = shard * seq_rows + jnp.arange(seq_rows, dtype=jnp.int32)
    placing = positions[:, None] == audio_pos[None, :]
    placed = jnp.dot(
        placing.astype(jnp.bfloat16), projected, preferred_element_type=jnp.float32
    ).astype(jnp.bfloat16)
    stream = jnp.where(jnp.any(placing, axis=1)[:, None], placed, text_embed)
    widened = stream.astype(jnp.float32)
    scaled = (widened * norm_gain).astype(jnp.bfloat16)
    sharers = chips // KVH
    quads = [[sharers * k + m for m in range(sharers)] for k in range(KVH)]
    strides = [[sharers * k + m for k in range(KVH)] for m in range(sharers)]
    shared = jnp.dot(scaled, by_head, preferred_element_type=jnp.float32).astype(jnp.bfloat16)
    shared = lax.all_to_all(
        shared.reshape(sharers, seq_rows // sharers, -1), "tp", 0, 0, axis_index_groups=quads, tiled=True
    )
    shared = shared.astype(jnp.float32).sum(axis=0).astype(jnp.bfloat16)
    shared = jnp.transpose(shared.reshape(seq_rows // sharers, KVH, 2 * HD), (1, 0, 2))
    shared = lax.all_to_all(shared, "tp", 0, 0, axis_index_groups=strides, tiled=True)
    shared = shared.astype(jnp.float32).sum(axis=0).astype(jnp.bfloat16)
    shared = lax.all_gather(shared, "tp", axis=0, tiled=True, axis_index_groups=quads)
    key_mine = shared[:, :HD]
    value_mine = shared[:, HD:]
    key_mine, value_mine, audio_pos, audio = lax.optimization_barrier(
        (key_mine, value_mine, audio_pos, audio)
    )
    all_rows = jnp.arange(key_segs.shape[0], dtype=jnp.int32)
    placing_all = all_rows[:, None] == audio_pos[None, :]
    is_audio = jnp.any(placing_all, axis=1)[:, None].astype(jnp.float32)
    heads_here = query_weight.shape[1] // HD
    query_sums, square_sums = query_partial(
        shard,
        gathered,
        audio,
        placing_all.astype(jnp.bfloat16),
        is_audio,
        query_weight.reshape(chips, 2, half, query_weight.shape[1]),
    )
    both_sums = jnp.concatenate([query_sums, square_sums], axis=1)
    own = lax.dynamic_slice_in_dim(both_sums, shard * seq_rows, seq_rows, 0)
    sent = lax.dynamic_slice_in_dim(both_sums, (1 - shard) * seq_rows, seq_rows, 0)
    own = own + swapped(sent)
    columns = query_weight.shape[1]
    inverse_rms = lax.rsqrt(jnp.sum(own[:, columns:], axis=1, keepdims=True) / D + norm_eps)
    query_raw = own[:, :columns] * inverse_rms
    queries = rotate(
        lax.optimization_barrier(query_raw.astype(jnp.bfloat16))
        .astype(jnp.float32)
        .reshape(seq_rows, heads_here, HD),
        positions,
    ).astype(jnp.bfloat16)
    key_mine = (key_mine.astype(jnp.float32) * inverse_rms).astype(jnp.bfloat16)
    value_mine = (value_mine.astype(jnp.float32) * inverse_rms).astype(jnp.bfloat16)
    key_rows = rotate(
        lax.optimization_barrier(key_mine).astype(jnp.float32)[:, None, :], positions
    )[:, 0, :].astype(jnp.bfloat16)
    both_rows = lax.all_gather(
        jnp.concatenate([key_rows, value_mine], axis=1), "sp", axis=0, tiled=True
    )
    key_block = both_rows[:, :HD]
    value_block = both_rows[:, HD:]
    inv_scale = 1.0 / math.sqrt(HD)
    running_max = jnp.full((heads_here, seq_rows), -1e30, jnp.float32)
    key_pos = jnp.arange(key_block.shape[0], dtype=jnp.int32)
    allowed = (key_pos[None, :] <= positions[:, None]) & (key_segs[None, :] == segment_ids[:, None])
    scores = (
        jnp.einsum("qhd,kd->hqk", queries, key_block, preferred_element_type=jnp.float32)
        * inv_scale
    )
    scores = jnp.where(allowed[None], scores, -1e30)
    new_max = jnp.maximum(running_max, jnp.max(scores, axis=2))
    expo = jnp.where(allowed[None], jnp.exp(scores - new_max[:, :, None]), 0.0)
    weight_sum = jnp.sum(expo, axis=2)
    accum = jnp.einsum(
        "hqk,kd->qhd", expo.astype(jnp.bfloat16), value_block, preferred_element_type=jnp.float32
    )
    running_max, weight_sum, accum = (new_max, weight_sum, accum)
    attended = (
        (accum / jnp.transpose(weight_sum)[:, :, None])
        .astype(jnp.bfloat16)
        .reshape(seq_rows, heads_here * HD)
    )
    block = output_weight
    mixed = jnp.transpose(
        lax.psum_scatter(
            jnp.einsum("hd,qh->dq", block, attended, preferred_element_type=jnp.float32).astype(
                jnp.bfloat16
            ),
            "tp",
            scatter_dimension=0,
            tiled=True,
        ).astype(jnp.float32)
    )
    return (widened + mixed).astype(jnp.bfloat16)


def solution(mesh):
    return jax.shard_map(
        per_device,
        mesh=mesh,
        in_specs=(
            P(("groups", "tp", "sp"), None),
            P(("groups", "tp", "sp")),
            P(("groups", "sp")),
            P(("groups", "sp"), "tp"),
            P(),
            P(),
            P(None, "tp"),
            P("tp"),
            P("tp", None),
            P(),
            P(),
            P(),
            P(None, "tp"),
            P("tp"),
            P(None, "tp"),
            P("tp", None),
            P("tp", None),
            P("tp", None),
        ),
        out_specs=P(("groups", "sp"), "tp"),
        check_vma=False,
    )
```
